16 devices in a mesh: fsdp: 16 (over z, y, x, core).
Axes of the slice: x: 2, y: 2, z: 2, core: 2. Of those that a mesh axis runs over, the one named last changes fastest.
Arguments:
- x: bfloat16 [4, 65536, 768], P(None, 'fsdp')
- g: bfloat16 [4, 65536, 768], P(None, 'fsdp')
- w1: bfloat16 [1, 768, 3072], P(None, 'fsdp')
- w2: bfloat16 [1, 3072, 768], P(None, 'fsdp')
Outputs:
- output 1: bfloat16 [4, 65536, 768], P(None, 'fsdp')
- output 2: float32 [1, 768, 3072], P(None, 'fsdp')
- output 3: float32 [1, 3072, 768], P(None, 'fsdp')
All inputs are finite; a program needn't handle non-finite values.
Results may differ from the reference program's by a relative error of at most 0.00940272.
Values are sent between devices in bfloat16 or wider.
A program may use at most 1 GiB of HBM per device.

```python
import jax
import jax.numpy as jnp
from jax import lax

D = 768
FF = 3072
LAYERS = 1
MICRO = 4
TOKENS = 65536


def setup_inputs(seed: int = 0) -> dict:
    k1, k2, k3, k4 = jax.random.split(jax.random.key(seed), 4)
    w1 = jax.random.normal(k1, (LAYERS, D, FF), jnp.float32) * D ** -0.5
    w2 = jax.random.normal(k2, (LAYERS, FF, D), jnp.float32) * FF ** -0.5
    x = jax.random.normal(k3, (MICRO, TOKENS, D), jnp.float32)
    g = jax.random.normal(k4, (MICRO, TOKENS, D), jnp.float32) * (MICRO * TOKENS) ** -0.5
    return {"x": x.astype(jnp.bfloat16), "g": g.astype(jnp.bfloat16),
            "w1": w1.astype(jnp.bfloat16), "w2": w2.astype(jnp.bfloat16)}


def _gelu_bwd(a, e):
    return jax.vjp(jax.nn.gelu, a)[1](e)[0]


def _micro(w1, w2, x, g):
    def fwd(xl, ws):
        v1, v2 = ws
        a = jnp.dot(xl, v1, preferred_element_type=jnp.float32).astype(jnp.bfloat16)
        h = jax.nn.gelu(a.astype(jnp.float32)).astype(jnp.bfloat16)
        y = (xl.astype(jnp.float32) + jnp.dot(h, v2, preferred_element_type=jnp.float32)).astype(jnp.bfloat16)
        return y, (xl, a)

    y, (xs, acts) = lax.scan(fwd, x, (w1, w2))

    def bwd(gy, inp):
        v1, v2, xl, a = inp
        h = jax.nn.gelu(a.astype(jnp.float32)).astype(jnp.bfloat16)
        e = jnp.dot(gy, v2.T, preferred_element_type=jnp.float32)
        da = _gelu_bwd(a.astype(jnp.float32), e).astype(jnp.bfloat16)
        dw2 = jnp.dot(h.T, gy, preferred_element_type=jnp.float32)
        dw1 = jnp.dot(xl.T, da, preferred_element_type=jnp.float32)
        gx = (gy.astype(jnp.float32) + jnp.dot(da, v1.T, preferred_element_type=jnp.float32)).astype(jnp.bfloat16)
        return gx, (dw1, dw2)

    _, (dw1, dw2) = lax.scan(bwd, g, (w1, w2, xs, acts), reverse=True)
    return y, dw1, dw2


def reference(x, g, w1, w2):
    def step(acc, xg):
        y, dw1, dw2 = _micro(w1, w2, xg[0], xg[1])
        return (acc[0] + dw1, acc[1] + dw2), y

    zeros = (jnp.zeros(w1.shape, jnp.float32), jnp.zeros(w2.shape, jnp.float32))
    (dw1, dw2), y = lax.scan(step, zeros, (x, g))
    return (y, dw1, dw2)
```

```python
import functools

import jax
import jax.numpy as jnp
from jax import lax
from jax.experimental import pallas as pl
from jax.experimental.pallas import tpu as pltpu
from jax.sharding import PartitionSpec as P

AX = "fsdp"
F32, BF16 = jnp.float32, jnp.bfloat16
C0 = 0.7978845608028654
C1 = 0.044715
VMEM_LIMIT = 66 * 1024 * 1024 - 2 * 1024 * 1024


def _half_cdf(af):
    sq = af * af
    return 0.5 + 0.5 * jnp.tanh(af * (C0 + (C0 * C1) * sq)), sq


def _dot(p, q, dims=((1,), (0,))):
    return lax.dot_general(p, q, (dims, ((), ())), preferred_element_type=F32)


def _fwd_kernel(fw, x_ref, g_ref, w1_ref, a_ref, h_ref, dw2_ref, acc_ref, sem):
    step, steps = pl.program_id(0), pl.num_programs(0)

    @pl.when(step == 0)
    def _():
        acc_ref[...] = jnp.zeros_like(acc_ref)

    for j in range(w1_ref.shape[1] // fw):
        c = pl.ds(j * fw, fw)
        a = _dot(x_ref[...], w1_ref[:, c]).astype(BF16)
        a_ref[:, c] = a
        af = a.astype(F32)
        s, _ = _half_cdf(af)
        h = (af * s).astype(BF16)
        h_ref[:, c] = h
        acc_ref[c, :] += _dot(h, g_ref[...], ((0,), (0,)))

    @pl.when(step == steps - 1)
    def _():
        copy = pltpu.make_async_copy(acc_ref, dw2_ref, sem)
        copy.start()
        copy.wait()


def _fwd(x, g, w1, tm, fw):
    t, d = x.shape
    ff = w1.shape[1]
    return pl.pallas_call(
        functools.partial(_fwd_kernel, fw),
        grid=(t // tm,),
        in_specs=[pl.BlockSpec((tm, d), lambda i: (i, 0)), pl.BlockSpec((tm, d), lambda i: (i, 0)),
                  pl.BlockSpec((d, ff), lambda i: (0, 0), pipeline_mode=pl.Buffered(1))],
        out_specs=[pl.BlockSpec((tm, ff), lambda i: (i, 0)), pl.BlockSpec((tm, ff), lambda i: (i, 0)),
                   pl.BlockSpec(memory_space=pl.ANY)],
        out_shape=[jax.ShapeDtypeStruct((t, ff), BF16), jax.ShapeDtypeStruct((t, ff), BF16),
                   jax.ShapeDtypeStruct((ff, d), F32)],
        scratch_shapes=[pltpu.VMEM((ff, d), F32), pltpu.SemaphoreType.DMA],
        compiler_params=pltpu.CompilerParams(dimension_semantics=("arbitrary",), vmem_limit_bytes=VMEM_LIMIT),
        cost_estimate=pl.CostEstimate(flops=4 * t * d * ff, bytes_accessed=4 * t * (d + ff), transcendentals=t * ff),
        name="fwd",
    )(x, g, w1)


def _bwd_kernel(fw, x_ref, g_ref, a_ref, w2_ref, dw1_ref, acc_ref, xt_ref, sem):
    step, steps = pl.program_id(0), pl.num_programs(0)

    @pl.when(step == 0)
    def _():
        acc_ref[...] = jnp.zeros_like(acc_ref)

    xt_ref[...] = x_ref[...].T
    for j in range(w2_ref.shape[0] // fw):
        c = pl.ds(j * fw, fw)
        e = _dot(g_ref[...], w2_ref[c, :], ((1,), (1,)))
        af = a_ref[:, c].astype(F32)
        s, sq = _half_cdf(af)
        dg = s + (af * s) * (1.0 - s) * ((2 * C0) + (6 * C0 * C1) * sq)
        da = (dg * e).astype(BF16)
        acc_ref[:, c] += _dot(xt_ref[...], da)

    @pl.when(step == steps - 1)
    def _():
        copy = pltpu.make_async_copy(acc_ref, dw1_ref, sem)
        copy.start()
        copy.wait()


def _bwd(x, g, a, w2, tm, fw):
    t, d = x.shape
    ff = w2.shape[0]
    return pl.pallas_call(
        functools.partial(_bwd_kernel, fw),
        grid=(t // tm,),
        in_specs=[pl.BlockSpec((tm, d), lambda i: (i, 0)), pl.BlockSpec((tm, d), lambda i: (i, 0)),
                  pl.BlockSpec((tm, ff), lambda i: (i, 0)),
                  pl.BlockSpec((ff, d), lambda i: (0, 0), pipeline_mode=pl.Buffered(1))],
        out_specs=pl.BlockSpec(memory_space=pl.ANY),
        out_shape=jax.ShapeDtypeStruct((d, ff), F32),
        scratch_shapes=[pltpu.VMEM((d, ff), F32), pltpu.VMEM((d, tm), BF16), pltpu.SemaphoreType.DMA],
        compiler_params=pltpu.CompilerParams(dimension_semantics=("arbitrary",), vmem_limit_bytes=VMEM_LIMIT),
        cost_estimate=pl.CostEstimate(flops=4 * t * d * ff, bytes_accessed=4 * t * d + 2 * t * ff, transcendentals=t * ff),
        name="bwd",
    )(x, g, a, w2)


def _out_kernel(x_ref, h_ref, w2_ref, y_ref):
    y_ref[...] = (x_ref[...].astype(F32) + _dot(h_ref[...], w2_ref[...])).astype(BF16)


def _out(x, h, w2, tm):
    t, d = x.shape
    ff = w2.shape[0]
    return pl.pallas_call(
        _out_kernel,
        grid=(t // tm,),
        in_specs=[pl.BlockSpec((tm, d), lambda i: (i, 0)), pl.BlockSpec((tm, ff), lambda i: (i, 0)),
                  pl.BlockSpec((ff, d), lambda i: (0, 0), pipeline_mode=pl.Buffered(1))],
        out_specs=pl.BlockSpec((tm, d), lambda i: (i, 0)),
        out_shape=jax.ShapeDtypeStruct((t, d), BF16),
        compiler_params=pltpu.CompilerParams(dimension_semantics=("arbitrary",), vmem_limit_bytes=VMEM_LIMIT),
        cost_estimate=pl.CostEstimate(flops=2 * t * d * ff, bytes_accessed=4 * t * d + 2 * t * ff, transcendentals=0),
        name="out",
    )(x, h, w2)


def solution(mesh):
    spec = P(None, AX, None)

    def body(x, g, w1, w2):
        shape, d = x.shape, x.shape[-1]
        xf, gf = x.reshape(-1, d), g.reshape(-1, d)
        v1 = lax.all_gather(w1[0], AX, axis=0, tiled=True)
        v2 = lax.all_gather(w2[0], AX, axis=0, tiled=True)
        a, h, p2 = _fwd(xf, gf, v1, 512, 512)
        d2 = lax.psum_scatter(p2, AX, scatter_dimension=0, tiled=True)
        p1 = _bwd(xf, gf, a, v2, 512, 512)
        d1 = lax.psum_scatter(p1, AX, scatter_dimension=0, tiled=True)
        h, p1 = lax.optimization_barrier((h, p1))
        y = _out(xf, h, v2, 512)
        return y.reshape(shape), d1[None], d2[None]

    return jax.shard_map(body, mesh=mesh, in_specs=(spec, spec, spec, spec),
                         out_specs=(spec, spec, spec), check_vma=False)
```

```python
import functools

import jax
import jax.numpy as jnp
from jax import lax
from jax.experimental import pallas as pl
from jax.experimental.pallas import tpu as pltpu
from jax.sharding import PartitionSpec as P

AX = "fsdp"
F32, BF16 = jnp.float32, jnp.bfloat16
C0 = 0.7978845608028654
C1 = 0.044715
TM = 1024
FW = 256
RB = 256
AB = 64
HEAD = 768
PARAMS = dict(dimension_semantics=("arbitrary",), vmem_limit_bytes=64 * 1024 * 1024 - 65536)


def _half_cdf(af):
    sq = af * af
    return 0.5 + 0.5 * jnp.tanh(af * (C0 + (C0 * C1) * sq)), sq


def _dot(p, q, dims=((1,), (0,))):
    return lax.dot_general(p, q, (dims, ((), ())), preferred_element_type=F32)


def _clear(ref):
    @pl.when(pl.program_id(0) == 0)
    def _():
        @pl.loop(0, ref.shape[0] // 8)
        def _(i):
            ref[pl.ds(pl.multiple_of(i * 8, 8), 8), :] = jnp.zeros((8, ref.shape[1]), F32)


def _flush(src, dst, sem):
    @pl.when(pl.program_id(0) == pl.num_programs(0) - 1)
    def _():
        copy = pltpu.make_async_copy(src, dst, sem)
        copy.start()
        copy.wait()


def _mix(matmuls, others):
    done = 0
    for i, piece in enumerate(matmuls):
        piece()
        while done < len(others) * (i + 1) // len(matmuls):
            others[done]()
            done += 1
    for piece in others[done:]:
        piece()


def _skewed(n, first, act, second, prologue=()):
    for j in range(n + 2):
        matmuls, others = [], list(prologue) if j == 0 else []
        if j < n:
            matmuls += first(j)
        if 0 <= j - 2 < n:
            matmuls += second(j - 2)
        if 0 <= j - 1 < n:
            others += act(j - 1)
        _mix(matmuls, others)


def _fwd_kernel(row0, *refs):
    x_ref, g_ref, w1_ref = refs[:3]
    a_ref, h_ref, dw2_ref, acc_ref, sem = refs[-5:]
    tm, ff = x_ref.shape[0], w1_ref.shape[1]
    _clear(acc_ref)

    def first(j):
        c = pl.ds(j * FW, FW)

        def piece(r):
            q = pl.ds(r * RB, RB)
            a_ref[q, c] = _dot(x_ref[q, :], w1_ref[:, c]).astype(BF16)

        return [functools.partial(piece, r) for r in range(tm // RB)]

    def act(j):
        c = pl.ds(j * FW, FW)

        def piece(r):
            q = pl.ds(r * AB, AB)
            af = a_ref[q, c].astype(F32)
            s, _ = _half_cdf(af)
            h_ref[q, c] = (af * s).astype(BF16)

        return [functools.partial(piece, r) for r in range(tm // AB)]

    def second(j):
        c = pl.ds(j * FW, FW)

        def piece():
            acc_ref[c, :] += _dot(h_ref[:, c], g_ref[...], ((0,), (0,)))

        return [piece]

    _skewed(ff // FW, first, act, second)
    _flush(acc_ref, dw2_ref.at[pl.ds(row0, ff), :], sem)


def _fwd(x, g, w1, row0, rows, dw2=None):
    (t, d), ff = x.shape, w1.shape[1]
    token = lambda n: pl.BlockSpec((TM, n), lambda i: (i, 0))
    hbm = pl.BlockSpec(memory_space=pl.ANY)
    more = [] if dw2 is None else [dw2]
    return pl.pallas_call(
        functools.partial(_fwd_kernel, row0),
        grid=(t // TM,),
        in_specs=[token(d), token(d), pl.BlockSpec((d, ff), lambda i: (0, 0), pipeline_mode=pl.Buffered(1))]
        + [hbm] * len(more),
        out_specs=[token(ff), token(ff), hbm],
        out_shape=[jax.ShapeDtypeStruct((t, ff), BF16), jax.ShapeDtypeStruct((t, ff), BF16),
                   jax.ShapeDtypeStruct((rows, d), F32)],
        scratch_shapes=[pltpu.VMEM((ff, d), F32), pltpu.SemaphoreType.DMA],
        input_output_aliases={3: 2} if more else {},
        compiler_params=pltpu.CompilerParams(**PARAMS),
        cost_estimate=pl.CostEstimate(flops=4 * t * d * ff, bytes_accessed=4 * t * (d + ff), transcendentals=t * ff),
        name="fwd",
    )(x, g, w1, *more)


def _bwd_kernel(x_ref, g_ref, a0_ref, a1_ref, w2_ref, dw1_ref, acc_ref, xt_ref, sem, e0, e1, b0, b1):
    tm, ff, head = x_ref.shape[0], w2_ref.shape[0], a0_ref.shape[1]
    es, das = (e0, e1), (b0, b1)
    _clear(acc_ref)

    def first(j):
        c = pl.ds(j * FW, FW)

        def piece(r):
            q = pl.ds(r * RB, RB)
            es[j % 2][q, :] = _dot(g_ref[q, :], w2_ref[c, :], ((1,), (1,)))

        return [functools.partial(piece, r) for r in range(tm // RB)]

    def act(j):
        col = j * FW
        a_ref, col = (a0_ref, col) if col < head else (a1_ref, col - head)

        def piece(r):
            q = pl.ds(r * AB, AB)
            af = a_ref[q, pl.ds(col, FW)].astype(F32)
            s, sq = _half_cdf(af)
            slope = s + (s * (1.0 - s)) * (af * ((2 * C0) + (6 * C0 * C1) * sq))
            das[j % 2][q, :] = (slope * es[j % 2][q, :]).astype(BF16)

        return [functools.partial(piece, r) for r in range(tm // AB)]

    def second(j):
        c = pl.ds(j * FW, FW)

        def piece():
            acc_ref[:, c] += _dot(xt_ref[...], das[j % 2][...])

        return [piece]

    def transpose(r):
        q = pl.ds(r * 128, 128)
        xt_ref[:, q] = x_ref[q, :].T

    _skewed(ff // FW, first, act, second, [functools.partial(transpose, r) for r in range(tm // 128)])
    _flush(acc_ref, dw1_ref, sem)


def _bwd(x, g, a0, a1, w2):
    (t, d), ff = x.shape, w2.shape[0]
    token = lambda n: pl.BlockSpec((TM, n), lambda i: (i, 0))
    return pl.pallas_call(
        _bwd_kernel,
        grid=(t // TM,),
        in_specs=[token(d), token(d), token(a0.shape[1]), token(a1.shape[1]),
                  pl.BlockSpec((ff, d), lambda i: (0, 0), pipeline_mode=pl.Buffered(1))],
        out_specs=pl.BlockSpec(memory_space=pl.ANY),
        out_shape=jax.ShapeDtypeStruct((d, ff), F32),
        scratch_shapes=[pltpu.VMEM((d, ff), F32), pltpu.VMEM((d, TM), BF16), pltpu.SemaphoreType.DMA]
        + [pltpu.VMEM((TM, FW), F32)] * 2 + [pltpu.VMEM((TM, FW), BF16)] * 2,
        compiler_params=pltpu.CompilerParams(**PARAMS),
        cost_estimate=pl.CostEstimate(flops=4 * t * d * ff, bytes_accessed=4 * t * d + 2 * t * ff, transcendentals=t * ff),
        name="bwd",
    )(x, g, a0, a1, w2)


def _out_kernel(x_ref, h0_ref, h1_ref, w2_ref, y_ref):
    head = h0_ref.shape[1]
    for r in range(x_ref.shape[0] // RB):
        q = pl.ds(r * RB, RB)
        z = _dot(h0_ref[q, :], w2_ref[:head, :]) + _dot(h1_ref[q, :], w2_ref[head:, :])
        y_ref[q, :] = (x_ref[q, :].astype(F32) + z).astype(BF16)


def _out(x, h0, h1, w2):
    (t, d), ff = x.shape, w2.shape[0]
    token = lambda n: pl.BlockSpec((TM, n), lambda i: (i, 0))
    return pl.pallas_call(
        _out_kernel,
        grid=(t // TM,),
        in_specs=[token(d), token(h0.shape[1]), token(h1.shape[1]),
                  pl.BlockSpec((ff, d), lambda i: (0, 0), pipeline_mode=pl.Buffered(1))],
        out_specs=token(d),
        out_shape=jax.ShapeDtypeStruct((t, d), BF16),
        compiler_params=pltpu.CompilerParams(**PARAMS),
        cost_estimate=pl.CostEstimate(flops=2 * t * d * ff, bytes_accessed=4 * t * d + 2 * t * ff, transcendentals=0),
        name="out",
    )(x, h0, h1, w2)


def solution(mesh):
    spec = P(None, AX, None)

    def body(x, g, w1, w2):
        shape, d = x.shape, x.shape[-1]
        xf, gf = x.reshape(-1, d), g.reshape(-1, d)
        gather = functools.partial(lax.all_gather, axis_name=AX, axis=0, tiled=True)
        scatter = functools.partial(lax.psum_scatter, axis_name=AX, scatter_dimension=0, tiled=True)
        v1a, v1b = gather(w1[0, :, :HEAD]), gather(w1[0, :, HEAD:])
        v2 = gather(w2[0])
        rows = v2.shape[0]
        a0, h0, p2 = _fwd(xf, gf, v1a, 0, rows)
        a1, h1, p2 = _fwd(xf, gf, v1b, HEAD, rows, p2)
        d2 = scatter(p2)
        p1 = _bwd(xf, gf, a0, a1, v2)
        d1 = scatter(p1)
        h0, h1, p1 = lax.optimization_barrier((h0, h1, p1))
        y = _out(xf, h0, h1, v2)
        return y.reshape(shape), d1[None], d2[None]

    return jax.shard_map(body, mesh=mesh, in_specs=(spec, spec, spec, spec),
                         out_specs=(spec, spec, spec), check_vma=False)
```

```python
import functools

import jax
import jax.numpy as jnp
from jax import lax
from jax.experimental import pallas as pl
from jax.experimental.pallas import tpu as pltpu
from jax.sharding import PartitionSpec as P

AX = "fsdp"
F32, BF16 = jnp.float32, jnp.bfloat16
C0 = 0.7978845608028654
C1 = 0.044715
TM = 1024
FW = 256
RB = 256
AB = 64
DEVICES = 16
HEAD = 768
PARAMS = dict(dimension_semantics=("arbitrary",), vmem_limit_bytes=64 * 1024 * 1024 - 65536)


def _half_cdf(af):
    sq = af * af
    return 0.5 + 0.5 * jnp.tanh(af * (C0 + (C0 * C1) * sq)), sq


def _dot(p, q, dims=((1,), (0,))):
    return lax.dot_general(p, q, (dims, ((), ())), preferred_element_type=F32)


def _clear(ref):
    @pl.when(pl.program_id(0) == 0)
    def _():
        rows = 16

        @pl.loop(0, ref.shape[0] // rows)
        def _(i):
            ref[pl.ds(pl.multiple_of(i * rows, rows), rows), :] = jnp.zeros((rows, ref.shape[1]), ref.dtype)


def _flush(src, dst, sem):
    @pl.when(pl.program_id(0) == pl.num_programs(0) - 1)
    def _():
        copy = pltpu.make_async_copy(src, dst, sem)
        copy.start()
        copy.wait()


def _gather_kernel(w_ref, out_ref, send, recv, pass_send, pass_recv):
    me = lax.axis_index(AX)
    flip = lambda b: 2**b * (1 - 2 * (me // 2**b % 2))
    other = me + flip(0)
    hops = (1, 2, 4, 3, 5, 6, 7)
    peers = {k: me + sum(flip(b + 1) for b in range(3) if k >> b & 1) for k in hops}

    barrier = pltpu.get_barrier_semaphore()
    for device in (other, *peers.values()):
        pl.semaphore_signal(barrier, inc=1, device_id=(device,), device_id_type=pl.DeviceIdType.MESH)
    pl.semaphore_wait(barrier, 1 + len(hops))

    def push(src, block, device, s, r):
        copy = pltpu.make_async_remote_copy(src_ref=src, dst_ref=out_ref.at[block], send_sem=s, recv_sem=r,
                                            device_id=(device,), device_id_type=pl.DeviceIdType.MESH)
        copy.start()
        return copy

    own = w_ref.at[0, :, pl.ds(0, out_ref.shape[2])]
    direct = {k: push(own, me, peers[k], send.at[k], recv.at[k]) for k in hops}
    passed = [push(own, me, other, pass_send.at[0], pass_recv.at[0])]
    out_ref[me] = own[...]
    for k in hops:
        direct[k].wait_recv()
        passed.append(push(out_ref.at[peers[k]], peers[k], other, pass_send.at[k], pass_recv.at[k]))
    for copy in passed:
        copy.wait_recv()
    for copy in (*direct.values(), *passed):
        copy.wait_send()


def _gather(w1, columns):
    rows = w1.shape[1]
    return pl.pallas_call(
        _gather_kernel,
        in_specs=[pl.BlockSpec(memory_space=pltpu.VMEM)],
        out_specs=pl.BlockSpec(memory_space=pltpu.VMEM),
        out_shape=jax.ShapeDtypeStruct((DEVICES, rows, columns), w1.dtype),
        scratch_shapes=[pltpu.SemaphoreType.DMA((8,))] * 4,
        compiler_params=pltpu.CompilerParams(collective_id=0, has_side_effects=True),
        name="gather",
    )(w1).reshape(DEVICES * rows, columns)


def _mix(matmuls, others):
    done = 0
    for i, piece in enumerate(matmuls):
        piece()
        while done < len(others) * (i + 1) // len(matmuls):
            others[done]()
            done += 1
    for piece in others[done:]:
        piece()


def _skewed(n, first, act, second, prologue=()):
    for j in range(n + 2):
        matmuls, others = [], list(prologue) if j == 0 else []
        if j < n:
            matmuls += first(j)
        if 0 <= j - 2 < n:
            matmuls += second(j - 2)
        if 0 <= j - 1 < n:
            others += act(j - 1)
        _mix(matmuls, others)


def _fwd_kernel(row0, col0, *refs):
    x_ref, g_ref, w1_ref = refs[:3]
    a_ref, h_ref, dw2_ref, acc_ref, sem = refs[-5:]
    tm, ff = a_ref.shape
    _clear(acc_ref)

    def first(j):
        c = pl.ds(j * FW, FW)

        def piece(r):
            q = pl.ds(r * RB, RB)
            a_ref[q, c] = _dot(x_ref[q, :], w1_ref[:, pl.ds(col0 + j * FW, FW)]).astype(BF16)

        return [functools.partial(piece, r) for r in range(tm // RB)]

    def act(j):
        c = pl.ds(j * FW, FW)

        def piece(r):
            q = pl.ds(r * AB, AB)
            af = a_ref[q, c].astype(F32)
            s, _ = _half_cdf(af)
            h_ref[q, c] = (af * s).astype(BF16)

        return [functools.partial(piece, r) for r in range(tm // AB)]

    def second(j):
        c = pl.ds(j * FW, FW)

        def piece():
            acc_ref[c, :] += _dot(h_ref[:, c], g_ref[...], ((0,), (0,)))

        return [piece]

    _skewed(ff // FW, first, act, second)
    _flush(acc_ref, dw2_ref.at[pl.ds(row0, ff), :], sem)


def _fwd(x, g, w1, col0, row0, rows, tm, dw2=None):
    (t, d), ff = x.shape, w1.shape[1] - col0
    token = lambda n: pl.BlockSpec((tm, n), lambda i: (i, 0))
    hbm = pl.BlockSpec(memory_space=pl.ANY)
    more = [] if dw2 is None else [dw2]
    return pl.pallas_call(
        functools.partial(_fwd_kernel, row0, col0),
        grid=(t // tm,),
        in_specs=[token(d), token(d), pl.BlockSpec(w1.shape, lambda i: (0, 0), pipeline_mode=pl.Buffered(1))]
        + [hbm] * len(more),
        out_specs=[token(ff), token(ff), hbm],
        out_shape=[jax.ShapeDtypeStruct((t, ff), BF16), jax.ShapeDtypeStruct((t, ff), BF16),
                   jax.ShapeDtypeStruct((rows, d), F32)],
        scratch_shapes=[pltpu.VMEM((ff, d), F32), pltpu.SemaphoreType.DMA],
        input_output_aliases={3: 2} if more else {},
        compiler_params=pltpu.CompilerParams(**PARAMS),
        cost_estimate=pl.CostEstimate(flops=4 * t * d * ff, bytes_accessed=4 * t * (d + ff), transcendentals=t * ff),
        name="fwd",
    )(x, g, w1, *more)


def _bwd_kernel(x_ref, g_ref, a0_ref, a1_ref, w2_ref, dw1_ref, acc_ref, xt_ref, sem, e0, e1, b0, b1):
    tm, ff, head = x_ref.shape[0], w2_ref.shape[0], a0_ref.shape[1]
    es, das = (e0, e1), (b0, b1)
    _clear(acc_ref)

    def first(j):
        c = pl.ds(j * FW, FW)

        def piece(r):
            q = pl.ds(r * RB, RB)
            es[j % 2][q, :] = _dot(g_ref[q, :], w2_ref[c, :], ((1,), (1,)))

        return [functools.partial(piece, r) for r in range(tm // RB)]

    def act(j):
        col = j * FW
        a_ref, col = (a0_ref, col) if col < head else (a1_ref, col - head)

        def piece(r):
            q = pl.ds(r * AB, AB)
            af = a_ref[q, pl.ds(col, FW)].astype(F32)
            s, sq = _half_cdf(af)
            slope = s + (s * (1.0 - s)) * (af * ((2 * C0) + (6 * C0 * C1) * sq))
            das[j % 2][q, :] = (slope * es[j % 2][q, :]).astype(BF16)

        return [functools.partial(piece, r) for r in range(tm // AB)]

    def second(j):
        c = pl.ds(j * FW, FW)

        def piece():
            acc_ref[:, c] += _dot(xt_ref[...], das[j % 2][...])

        return [piece]

    def transpose(r):
        q = pl.ds(r * 128, 128)
        xt_ref[:, q] = x_ref[q, :].T

    _skewed(ff // FW, first, act, second, [functools.partial(transpose, r) for r in range(tm // 128)])
    _flush(acc_ref, dw1_ref, sem)


def _bwd(x, g, a0, a1, w2):
    (t, d), ff = x.shape, w2.shape[0]
    token = lambda n: pl.BlockSpec((TM, n), lambda i: (i, 0))
    return pl.pallas_call(
        _bwd_kernel,
        grid=(t // TM,),
        in_specs=[token(d), token(d), token(a0.shape[1]), token(a1.shape[1]),
                  pl.BlockSpec((ff, d), lambda i: (0, 0), pipeline_mode=pl.Buffered(1))],
        out_specs=pl.BlockSpec(memory_space=pl.ANY),
        out_shape=jax.ShapeDtypeStruct((d, ff), F32),
        scratch_shapes=[pltpu.VMEM((d, ff), F32), pltpu.VMEM((d, TM), BF16), pltpu.SemaphoreType.DMA]
        + [pltpu.VMEM((TM, FW), F32)] * 2 + [pltpu.VMEM((TM, FW), BF16)] * 2,
        compiler_params=pltpu.CompilerParams(**PARAMS),
        cost_estimate=pl.CostEstimate(flops=4 * t * d * ff, bytes_accessed=4 * t * d + 2 * t * ff, transcendentals=t * ff),
        name="bwd",
    )(x, g, a0, a1, w2)


def _out_kernel(x_ref, h0_ref, h1_ref, w2_ref, y_ref):
    head = h0_ref.shape[1]
    for r in range(x_ref.shape[0] // RB):
        q = pl.ds(r * RB, RB)
        z = _dot(h0_ref[q, :], w2_ref[:head, :]) + _dot(h1_ref[q, :], w2_ref[head:, :])
        y_ref[q, :] = (x_ref[q, :].astype(F32) + z).astype(BF16)


def _out(x, h0, h1, w2):
    (t, d), ff = x.shape, w2.shape[0]
    token = lambda n: pl.BlockSpec((TM, n), lambda i: (i, 0))
    return pl.pallas_call(
        _out_kernel,
        grid=(t // TM,),
        in_specs=[token(d), token(h0.shape[1]), token(h1.shape[1]),
                  pl.BlockSpec((ff, d), lambda i: (0, 0), pipeline_mode=pl.Buffered(1))],
        out_specs=token(d),
        out_shape=jax.ShapeDtypeStruct((t, d), BF16),
        compiler_params=pltpu.CompilerParams(**PARAMS),
        cost_estimate=pl.CostEstimate(flops=2 * t * d * ff, bytes_accessed=4 * t * d + 2 * t * ff, transcendentals=0),
        name="out",
    )(x, h0, h1, w2)


def solution(mesh):
    spec = P(None, AX, None)

    def body(x, g, w1, w2):
        shape, d = x.shape, x.shape[-1]
        xf, gf = x.reshape(-1, d), g.reshape(-1, d)
        gather = functools.partial(lax.all_gather, axis_name=AX, axis=0, tiled=True)
        scatter = functools.partial(lax.psum_scatter, axis_name=AX, scatter_dimension=0, tiled=True)
        v1a = _gather(w1, HEAD)
        v1a, w1b, w2 = lax.optimization_barrier((v1a, w1[0, :, HEAD:], w2))
        v1b, v2 = gather(w1b), gather(w2[0])
        rows = v2.shape[0]
        a0, h0, p2 = _fwd(xf, gf, v1a, 0, 0, rows, 2 * TM)
        a1, h1, p2 = _fwd(xf, gf, v1b, 0, HEAD, rows, TM, p2)
        d2 = scatter(p2)
        p1 = _bwd(xf, gf, a0, a1, v2)
        d1 = scatter(p1)
        h0, h1, p1 = lax.optimization_barrier((h0, h1, p1))
        y = _out(xf, h0, h1, v2)
        return y.reshape(shape), d1[None], d2[None]

    return jax.shard_map(body, mesh=mesh, in_specs=(spec, spec, spec, spec),
                         out_specs=(spec, spec, spec), check_vma=False)
```

```python
import functools

import jax
import jax.numpy as jnp
from jax import lax
from jax.experimental import pallas as pl
from jax.experimental.pallas import tpu as pltpu
from jax.sharding import PartitionSpec as P

AX = "fsdp"
F32, BF16 = jnp.float32, jnp.bfloat16
C0 = 0.7978845608028654
C1 = 0.044715
TM = 1024
FW = 256
RB = 256
AB = 64
DEVICES = 16
HEAD = 768
PARAMS = dict(dimension_semantics=("arbitrary",), vmem_limit_bytes=64 * 1024 * 1024 - 65536)


def _half_cdf(af):
    sq = af * af
    return 0.5 + 0.5 * jnp.tanh(af * (C0 + (C0 * C1) * sq)), sq


def _dot(p, q, dims=((1,), (0,))):
    return lax.dot_general(p, q, (dims, ((), ())), preferred_element_type=F32)


def _clear(ref):
    @pl.when(pl.program_id(0) == 0)
    def _():
        rows = 16

        @pl.loop(0, ref.shape[0] // rows)
        def _(i):
            ref[pl.ds(pl.multiple_of(i * rows, rows), rows), :] = jnp.zeros((rows, ref.shape[1]), ref.dtype)


def _flush(src, dst, sem):
    @pl.when(pl.program_id(0) == pl.num_programs(0) - 1)
    def _():
        copy = pltpu.make_async_copy(src, dst, sem)
        copy.start()
        copy.wait()


def _gather_kernel(w_ref, out_ref, rest_ref, send, recv, pass_send, pass_recv):
    me = lax.axis_index(AX)
    flip = lambda b: 2**b * (1 - 2 * (me // 2**b % 2))
    other = me + flip(0)
    hops = (1, 2, 4, 3, 5, 6, 7)
    peers = {k: me + sum(flip(b + 1) for b in range(3) if k >> b & 1) for k in hops}

    barrier = pltpu.get_barrier_semaphore()
    for device in (other, *peers.values()):
        pl.semaphore_signal(barrier, inc=1, device_id=(device,), device_id_type=pl.DeviceIdType.MESH)
    pl.semaphore_wait(barrier, 1 + len(hops))

    def push(src, block, device, s, r):
        copy = pltpu.make_async_remote_copy(src_ref=src, dst_ref=out_ref.at[block], send_sem=s, recv_sem=r,
                                            device_id=(device,), device_id_type=pl.DeviceIdType.MESH)
        copy.start()
        return copy

    own = w_ref.at[0, :, pl.ds(0, out_ref.shape[2])]
    direct = {k: push(own, me, peers[k], send.at[k], recv.at[k]) for k in hops}
    passed = [push(own, me, other, pass_send.at[0], pass_recv.at[0])]
    out_ref[me] = own[...]
    rest_ref[...] = w_ref[:, :, out_ref.shape[2]:]
    for k in hops:
        direct[k].wait_recv()
        passed.append(push(out_ref.at[peers[k]], peers[k], other, pass_send.at[k], pass_recv.at[k]))
    for copy in passed:
        copy.wait_recv()
    for copy in (*direct.values(), *passed):
        copy.wait_send()


def _gather(w1, columns):
    _, rows, ff = w1.shape
    vmem = pl.BlockSpec(memory_space=pltpu.VMEM)
    whole, rest = pl.pallas_call(
        _gather_kernel,
        in_specs=[vmem],
        out_specs=[vmem, vmem],
        out_shape=[jax.ShapeDtypeStruct((DEVICES, rows, columns), w1.dtype),
                   jax.ShapeDtypeStruct((1, rows, ff - columns), w1.dtype)],
        scratch_shapes=[pltpu.SemaphoreType.DMA((8,))] * 4,
        compiler_params=pltpu.CompilerParams(collective_id=0, has_side_effects=True),
        name="gather",
    )(w1)
    return whole.reshape(DEVICES * rows, columns), rest


def _mix(matmuls, others):
    done = 0
    for i, piece in enumerate(matmuls):
        piece()
        while done < len(others) * (i + 1) // len(matmuls):
            others[done]()
            done += 1
    for piece in others[done:]:
        piece()


def _skewed(n, first, act, second, prologue=(), second_leads=False):
    for j in range(n + 2):
        ahead, others = first(j) if j < n else [], list(prologue) if j == 0 else []
        behind = second(j - 2) if 0 <= j - 2 < n else []
        matmuls = behind + ahead if second_leads else ahead + behind
        if 0 <= j - 1 < n:
            others += act(j - 1)
        _mix(matmuls, others)


def _fwd_kernel(row0, col0, *refs):
    x_ref, g_ref, w1_ref = refs[:3]
    a_ref, h_ref, dw2_ref, acc_ref, sem = refs[-5:]
    tm, ff = a_ref.shape
    _clear(acc_ref)

    def first(j):
        c = pl.ds(j * FW, FW)

        def piece(r):
            q = pl.ds(r * RB, RB)
            a_ref[q, c] = _dot(x_ref[q, :], w1_ref[:, pl.ds(col0 + j * FW, FW)]).astype(BF16)

        return [functools.partial(piece, r) for r in range(tm // RB)]

    def act(j):
        c = pl.ds(j * FW, FW)

        def piece(r):
            q = pl.ds(r * AB, AB)
            af = a_ref[q, c].astype(F32)
            s, _ = _half_cdf(af)
            h_ref[q, c] = (af * s).astype(BF16)

        return [functools.partial(piece, r) for r in range(tm // AB)]

    def second(j):
        c = pl.ds(j * FW, FW)

        def piece():
            acc_ref[c, :] += _dot(h_ref[:, c], g_ref[...], ((0,), (0,)))

        return [piece]

    _skewed(ff // FW, first, act, second)
    _flush(acc_ref, dw2_ref.at[pl.ds(row0, ff), :], sem)


def _fwd(x, g, w1, col0, row0, rows, tm, dw2=None):
    (t, d), ff = x.shape, w1.shape[1] - col0
    token = lambda n: pl.BlockSpec((tm, n), lambda i: (i, 0))
    hbm = pl.BlockSpec(memory_space=pl.ANY)
    more = [] if dw2 is None else [dw2]
    return pl.pallas_call(
        functools.partial(_fwd_kernel, row0, col0),
        grid=(t // tm,),
        in_specs=[token(d), token(d), pl.BlockSpec(w1.shape, lambda i: (0, 0), pipeline_mode=pl.Buffered(1))]
        + [hbm] * len(more),
        out_specs=[token(ff), token(ff), hbm],
        out_shape=[jax.ShapeDtypeStruct((t, ff), BF16), jax.ShapeDtypeStruct((t, ff), BF16),
                   jax.ShapeDtypeStruct((rows, d), F32)],
        scratch_shapes=[pltpu.VMEM((ff, d), F32), pltpu.SemaphoreType.DMA],
        input_output_aliases={3: 2} if more else {},
        compiler_params=pltpu.CompilerParams(**PARAMS),
        cost_estimate=pl.CostEstimate(flops=4 * t * d * ff, bytes_accessed=4 * t * (d + ff), transcendentals=t * ff),
        name="fwd",
    )(x, g, w1, *more)


def _bwd_kernel(x_ref, g_ref, a0_ref, a1_ref, w2_ref, dw1_ref, acc_ref, xt_ref, sem, e0, e1, b0, b1):
    tm, ff, head = x_ref.shape[0], w2_ref.shape[0], a0_ref.shape[1]
    es, das = (e0, e1), (b0, b1)
    _clear(acc_ref)

    def first(j):
        c = pl.ds(j * FW, FW)

        def piece(r):
            q = pl.ds(r * 2 * RB, 2 * RB)
            es[j % 2][q, :] = _dot(g_ref[q, :], w2_ref[c, :], ((1,), (1,)))

        return [functools.partial(piece, r) for r in range(tm // (2 * RB))]

    def act(j):
        col = j * FW
        a_ref, col = (a0_ref, col) if col < head else (a1_ref, col - head)

        def piece(r):
            q = pl.ds(r * AB, AB)
            af = a_ref[q, pl.ds(col, FW)].astype(F32)
            s, sq = _half_cdf(af)
            slope = s + (s * (1.0 - s)) * (af * ((2 * C0) + (6 * C0 * C1) * sq))
            das[j % 2][q, :] = (slope * es[j % 2][q, :]).astype(BF16)

        return [functools.partial(piece, r) for r in range(tm // AB)]

    def second(j):
        c = pl.ds(j * FW, FW)

        def piece():
            acc_ref[:, c] += _dot(xt_ref[...], das[j % 2][...])

        return [piece]

    def transpose(r):
        q = pl.ds(r * 128, 128)
        xt_ref[:, q] = x_ref[q, :].T

    _skewed(ff // FW, first, act, second, [functools.partial(transpose, r) for r in range(tm // 128)], True)
    _flush(acc_ref, dw1_ref, sem)


def _bwd(x, g, a0, a1, w2):
    (t, d), ff = x.shape, w2.shape[0]
    token = lambda n: pl.BlockSpec((TM, n), lambda i: (i, 0))
    return pl.pallas_call(
        _bwd_kernel,
        grid=(t // TM,),
        in_specs=[token(d), token(d), token(a0.shape[1]), token(a1.shape[1]),
                  pl.BlockSpec((ff, d), lambda i: (0, 0), pipeline_mode=pl.Buffered(1))],
        out_specs=pl.BlockSpec(memory_space=pl.ANY),
        out_shape=jax.ShapeDtypeStruct((d, ff), F32),
        scratch_shapes=[pltpu.VMEM((d, ff), F32), pltpu.VMEM((d, TM), BF16), pltpu.SemaphoreType.DMA]
        + [pltpu.VMEM((TM, FW), F32)] * 2 + [pltpu.VMEM((TM, FW), BF16)] * 2,
        compiler_params=pltpu.CompilerParams(**PARAMS),
        cost_estimate=pl.CostEstimate(flops=4 * t * d * ff, bytes_accessed=4 * t * d + 2 * t * ff, transcendentals=t * ff),
        name="bwd",
    )(x, g, a0, a1, w2)


def _out_kernel(x_ref, h0_ref, h1_ref, w2_ref, y_ref):
    head = h0_ref.shape[1]
    for r in range(x_ref.shape[0] // RB):
        q = pl.ds(r * RB, RB)
        z = _dot(h0_ref[q, :], w2_ref[:head, :]) + _dot(h1_ref[q, :], w2_ref[head:, :])
        y_ref[q, :] = (x_ref[q, :].astype(F32) + z).astype(BF16)


def _out(x, h0, h1, w2):
    (t, d), ff = x.shape, w2.shape[0]
    token = lambda n: pl.BlockSpec((TM, n), lambda i: (i, 0))
    return pl.pallas_call(
        _out_kernel,
        grid=(t // TM,),
        in_specs=[token(d), token(h0.shape[1]), token(h1.shape[1]),
                  pl.BlockSpec((ff, d), lambda i: (0, 0), pipeline_mode=pl.Buffered(1))],
        out_specs=token(d),
        out_shape=jax.ShapeDtypeStruct((t, d), BF16),
        compiler_params=pltpu.CompilerParams(**PARAMS),
        cost_estimate=pl.CostEstimate(flops=2 * t * d * ff, bytes_accessed=4 * t * d + 2 * t * ff, transcendentals=0),
        name="out",
    )(x, h0, h1, w2)


def solution(mesh):
    spec = P(None, AX, None)

    def body(x, g, w1, w2):
        shape, d = x.shape, x.shape[-1]
        xf, gf = x.reshape(-1, d), g.reshape(-1, d)
        gather = functools.partial(lax.all_gather, axis_name=AX, axis=0, tiled=True)
        scatter = functools.partial(lax.psum_scatter, axis_name=AX, scatter_dimension=0, tiled=True)
        v1a, w1b = _gather(w1, HEAD)
        w1b, w2 = lax.optimization_barrier((w1b, w2))
        v1b, v2 = gather(w1b[0]), gather(w2[0])
        rows = v2.shape[0]
        a0, h0, p2 = _fwd(xf, gf, v1a, 0, 0, rows, 2 * TM)
        a1, h1, p2 = _fwd(xf, gf, v1b, 0, HEAD, rows, TM, p2)
        d2 = scatter(p2)
        p1 = _bwd(xf, gf, a0, a1, v2)
        d1 = scatter(p1)
        h0, h1, p1 = lax.optimization_barrier((h0, h1, p1))
        y = _out(xf, h0, h1, v2)
        return y.reshape(shape), d1[None], d2[None]

    return jax.shard_map(body, mesh=mesh, in_specs=(spec, spec, spec, spec),
                         out_specs=(spec, spec, spec), check_vma=False)
```
